32 devices in a mesh: prompt: 4 (over x, core), dp: 4 (over z), mp: 2 (over y).
Axes of the slice: x: 2, y: 2, z: 4, core: 2. Of those that a mesh axis runs over, the one named last changes fastest.
Arguments:
- prompts: bfloat16 [8, 100, 4096], P('prompt'), may hold values from -6 to 6
- target_embed: bfloat16 [4, 512, 4096], P('dp'), may hold values from -6 to 6
- labels: int32 [4, 512], P('dp'), may hold values from 0 to 16383
- lengths: int32 [4], P('dp'), may hold values from 128 to 512
- attn_gain: float32 [4096], replicated, may hold values from 0.5 to 1.5
- w_qkv: bfloat16 [3, 4096, 2048], P(None, None, 'mp'), may hold values from -4 to 4
- w_out: bfloat16 [2048, 4096], P('mp'), may hold values from -0.5 to 0.5
- final_gain: float32 [4096], replicated, may hold values from 0.5 to 1.5
- w_vocab: bfloat16 [4096, 16384], P(None, ('dp', 'mp')), may hold values from -3 to 3
Outputs:
- token_loss: float32 [8, 4, 512], P('prompt', 'dp')
- prompt_loss: float32 [8], replicated
The draws below stay inside these ranges and needn't reach their ends.
Inputs may be any that keep to these rules, and one draw needn't show every extreme that they name: `lengths`: positions from a sequence's length on are padding.
All inputs are finite; a program needn't handle non-finite values.
Results may differ from the reference program's by a relative error of at most 0.006.
Values may be sent and summed in bfloat16 or wider, within the bound.
A program may use at most 192 MiB of HBM per device.

```python
import math
import jax
import jax.numpy as jnp
from jax import lax

D = 4096
HEADS = 16
HD = 128
V = 16384
LP = 100
S = 512
P_SIZE = 8
B = 4
N_MP = 2


def draw_w_qkv(key, part):
    noise = jnp.clip(jax.random.normal(key, (3, D, HEADS * HD), jnp.float32), -6.0, 6.0) / math.sqrt(D)
    return jnp.clip(noise, -4.0, 4.0).astype(jnp.bfloat16)


def draw_w_vocab(key, part):
    noise = jnp.clip(jax.random.normal(key, (D, V), jnp.float32), -6.0, 6.0)
    return (noise * 0.0625).astype(jnp.bfloat16)


def with_ends(drawn, own_key, low, top_value):
    spot = [jax.random.randint(jax.random.fold_in(own_key, axis), (), 0, length) for axis, length in enumerate(drawn.shape)]
    widest = drawn.shape.index(max(drawn.shape))
    neighbour = spot[:widest] + [(spot[widest] + 1) % drawn.shape[widest]] + spot[widest + 1:]
    return drawn.at[tuple(spot)].set(low).at[tuple(neighbour)].set(top_value)


def levels(stream_key, extent, cuts, smallest, top_value):
    loudness = 1.0
    for position, parts in cuts:
        heights = jax.random.uniform(jax.random.fold_in(jax.random.fold_in(stream_key, 6), position), (parts,), jnp.float32, smallest / len(cuts), top_value / len(cuts))
        loudness = loudness * jnp.repeat(jnp.exp(heights), extent[position] // parts).reshape((-1,) + (1,) * (len(extent) - 1 - position))
    return loudness


def bell_draw(key, extent, width, bound, split=(), kind=jnp.bfloat16):
    level = levels(key, extent, split, -0.22, 0.18) if split else 1.0
    result = jax.random.normal(key, extent, jnp.float32) * width * level
    return jnp.minimum(jnp.maximum(result, -bound), bound).astype(kind)


def setup_inputs(seed: int = 0) -> dict:
    keys = jax.random.split(jax.random.key(seed), 10)
    prompts = bell_draw(keys[0], (P_SIZE, LP, D), 1.0, 6.0, ((0, 4),))
    target_embed = bell_draw(keys[1], (B, S, D), 1.0, 6.0, ((0, 4),))
    labels = with_ends(jax.random.randint(keys[2], (B, S), 0, V), jax.random.fold_in(keys[2], 1), 0, V - 1).astype(jnp.int32)
    lengths = with_ends(jax.random.randint(keys[3], (B,), S // 4, S + 1), jax.random.fold_in(keys[3], 1), S // 4, S).astype(jnp.int32)
    attn_gain = jnp.clip(1.0 + 0.1 * jax.random.normal(keys[4], (D,), jnp.float32), 0.5, 1.5)
    w_qkv = draw_w_qkv(jax.random.fold_in(keys[9], 71), 0)
    w_out = bell_draw(keys[6], (HEADS * HD, D), (HEADS * HD // 16) ** -0.5, 0.5, ((0, 2),))
    final_gain = jnp.clip(1.0 + 0.1 * jax.random.normal(keys[7], (D,), jnp.float32), 0.5, 1.5)
    w_vocab = draw_w_vocab(jax.random.fold_in(keys[9], 71), 0)
    return {"prompts": prompts, "target_embed": target_embed, "labels": labels, "lengths": lengths, "attn_gain": attn_gain, "w_qkv": w_qkv, "w_out": w_out, "final_gain": final_gain, "w_vocab": w_vocab}


EPSILON = 1e-05
BASE_THETA = 10000.0

def rms_scaled(values, gain_vec):
    widened = values.astype(jnp.float32)
    return widened * lax.rsqrt(lax.optimization_barrier(jnp.mean(widened * widened, axis=-1, keepdims=True)) + EPSILON) * gain_vec

def rotate(values, offset, head_dim):
    number_rows = values.shape[-2]
    full_width = values.shape[-1]
    per_head = values.reshape(values.shape[:-1] + (full_width // head_dim, head_dim))
    half_dim = head_dim // 2
    positions = (offset + jnp.arange(number_rows, dtype=jnp.int32)).astype(jnp.float32)
    indices_f = jnp.arange(half_dim, dtype=jnp.int32).astype(jnp.float32)
    frequency = jnp.exp(indices_f * (-2.0 * math.log(BASE_THETA) / head_dim))
    angles = positions[:, None] * frequency[None, :]
    cosine = jnp.cos(angles)[:, None, :]
    sine_part = jnp.sin(angles)[:, None, :]
    first_half = per_head[..., :half_dim]
    second_half = per_head[..., half_dim:]
    turned = jnp.concatenate([first_half * cosine - second_half * sine_part, second_half * cosine + first_half * sine_part], axis=-1)
    return turned.reshape(values.shape)

def attend(prompt_keys, prompt_vals, target_q, target_k, target_v):
    seq_count = target_q.shape[0]
    target_len = target_q.shape[1]
    prompt_len = prompt_keys.shape[0]
    heads_here = target_q.shape[2] // HD
    keys_all = jnp.concatenate([jnp.broadcast_to(prompt_keys[None], (seq_count,) + prompt_keys.shape), target_k], axis=1)
    vals_all = jnp.concatenate([jnp.broadcast_to(prompt_vals[None], (seq_count,) + prompt_vals.shape), target_v], axis=1)
    query_h = target_q.reshape(seq_count, target_len, heads_here, HD).astype(jnp.float32)
    key_h = keys_all.reshape(seq_count, prompt_len + target_len, heads_here, HD).astype(jnp.float32)
    val_h = vals_all.reshape(seq_count, prompt_len + target_len, heads_here, HD).astype(jnp.float32)
    scores = jnp.einsum('bqhe,bkhe->bhqk', query_h, key_h) * HD ** (-0.5)
    key_index = jnp.arange(prompt_len + target_len, dtype=jnp.int32)
    query_pos = prompt_len + jnp.arange(target_len, dtype=jnp.int32)
    allowed = key_index[None, :] <= query_pos[:, None]
    scores = jnp.where(allowed[None, None], scores, -1e+30)
    top_val = lax.optimization_barrier(jnp.max(scores, axis=-1, keepdims=True))
    expo = jnp.exp(scores - top_val)
    probs = (expo / lax.optimization_barrier(jnp.sum(expo, axis=-1, keepdims=True))).astype(jnp.bfloat16)
    context = jnp.einsum('bhqk,bkhe->bqhe', probs.astype(jnp.float32), val_h)
    return context.astype(jnp.bfloat16).reshape(seq_count, target_len, heads_here * HD)

def reference(prompts, target_embed, labels, lengths, attn_gain, w_qkv, w_out, final_gain, w_vocab):
    seq_count = target_embed.shape[0]
    full_width = w_qkv.shape[2]
    group_width = full_width // N_MP
    normed_target = rms_scaled(target_embed, attn_gain).astype(jnp.bfloat16)
    flat_target = normed_target.reshape(-1, D)

    def linear(rows_in, index_w):
        return jnp.dot(rows_in, w_qkv[index_w], preferred_element_type=jnp.float32).reshape(seq_count, S, full_width)
    target_q = rotate(linear(flat_target, 0), LP, HD).astype(jnp.bfloat16)
    target_k = rotate(linear(flat_target, 1), LP, HD).astype(jnp.bfloat16)
    target_v = linear(flat_target, 2).astype(jnp.bfloat16)
    normed_prompts = rms_scaled(prompts, attn_gain).astype(jnp.bfloat16)
    residual = target_embed.reshape(-1, D).astype(jnp.float32)
    valid = jnp.arange(S, dtype=jnp.int32)[None, :] < lengths[:, None]
    flat_labels = labels.reshape(-1, 1)

    def one_prompt(prompt_rows):
        prompt_k = rotate(jnp.dot(prompt_rows, w_qkv[1], preferred_element_type=jnp.float32), 0, HD).astype(jnp.bfloat16)
        prompt_v = jnp.dot(prompt_rows, w_qkv[2], preferred_element_type=jnp.float32).astype(jnp.bfloat16)
        context = attend(prompt_k, prompt_v, target_q, target_k, target_v)
        ctx_flat = context.reshape(-1, full_width)
        hidden = residual
        for group in range(N_MP):
            part = jnp.dot(ctx_flat[:, group * group_width:(group + 1) * group_width], w_out[group * group_width:(group + 1) * group_width], preferred_element_type=jnp.float32).astype(jnp.bfloat16)
            part = lax.optimization_barrier(part)
            hidden = hidden + part.astype(jnp.float32)
        normed_out = rms_scaled(hidden, final_gain).astype(jnp.bfloat16)
        logits = jnp.dot(normed_out, w_vocab, preferred_element_type=jnp.float32)
        top_val = lax.optimization_barrier(jnp.max(logits, axis=1))
        log_total = top_val + jnp.log(lax.optimization_barrier(jnp.sum(jnp.exp(logits - top_val[:, None]), axis=1)))
        picked = jnp.take_along_axis(logits, flat_labels, axis=1)[:, 0]
        losses = (log_total - picked).reshape(seq_count, S)
        return jnp.where(valid, losses, 0.0)
    token_loss = lax.map(one_prompt, normed_prompts)
    prompt_loss = lax.optimization_barrier(jnp.sum(token_loss, axis=(1, 2))) / jnp.sum(lengths).astype(jnp.float32)
    return (token_loss, prompt_loss)
```

```python
import math

import jax
import jax.numpy as jnp
from jax import lax
from jax.sharding import PartitionSpec as P

HD = 128


EPSILON = 1e-05
BASE_THETA = 10000.0


def shift_by(value, axis, hop):
    size = lax.axis_size(axis)
    return lax.ppermute(value, axis, [(i, (i + hop) % size) for i in range(size)])


def ring_source(axis, hop):
    size = lax.axis_size(axis)
    return lax.rem(lax.axis_index(axis) + size - hop, size)


def in_order(parts, axis):
    size = len(parts)
    stacked = jnp.stack(parts)
    owners = lax.axis_index(axis) + size - jnp.arange(size, dtype=jnp.int32)
    return jnp.take(stacked, lax.rem(owners, size), axis=0)


def small_gather(value, axis):
    size = lax.axis_size(axis)
    return in_order([value] + [shift_by(value, axis, k) for k in range(1, size)], axis)


def spread_rows(piece, axis):
    size = lax.axis_size(axis)
    if size & (size - 1):
        return lax.all_gather(piece, axis, axis=0, tiled=True)
    me = lax.axis_index(axis)
    held = [(piece, me)]
    bit = size // 2
    while bit:
        pairs = [(i, i ^ bit) for i in range(size)]
        held = held + [
            (lax.ppermute(part, axis, pairs), jnp.bitwise_xor(owner, bit)) for part, owner in held
        ]
        bit //= 2
    height = piece.shape[0]
    whole = jnp.zeros((size * height,) + piece.shape[1:], piece.dtype)
    for part, owner in held:
        whole = lax.dynamic_update_slice_in_dim(whole, part, owner * height, 0)
    return whole


def peer_piece(weights):
    height = weights.shape[0] // lax.axis_size("prompt")
    return lax.dynamic_slice_in_dim(weights, lax.axis_index("prompt") * height, height, 0)


def rms_scaled(values, gain_vec):
    widened = values.astype(jnp.float32)
    return (
        widened
        * lax.rsqrt(jnp.mean(widened * widened, axis=-1, keepdims=True) + EPSILON)
        * gain_vec
    )


def rotate(values, offset, head_dim):
    number_rows = values.shape[-2]
    full_width = values.shape[-1]
    per_head = values.reshape(values.shape[:-1] + (full_width // head_dim, head_dim))
    half_dim = head_dim // 2
    positions = (offset + jnp.arange(number_rows, dtype=jnp.int32)).astype(jnp.float32)
    indices_f = jnp.arange(half_dim, dtype=jnp.int32).astype(jnp.float32)
    frequency = jnp.exp(indices_f * (-2.0 * math.log(BASE_THETA) / head_dim))
    angles = positions[:, None] * frequency[None, :]
    cosine = jnp.cos(angles)[:, None, :]
    sine_part = jnp.sin(angles)[:, None, :]
    first_half = per_head[..., :half_dim]
    second_half = per_head[..., half_dim:]
    turned = jnp.concatenate(
        [
            first_half * cosine - second_half * sine_part,
            second_half * cosine + first_half * sine_part,
        ],
        axis=-1,
    )
    return turned.reshape(values.shape)


def project(normed, weights, offset, rotated_count):
    lead_shape = normed.shape[:-1]
    flat_rows = normed.reshape(-1, normed.shape[-1])
    stacked = jnp.einsum("nd,cde->cne", flat_rows, weights, preferred_element_type=jnp.float32)
    stacked = stacked.reshape((weights.shape[0],) + lead_shape + (weights.shape[2],))
    results = []
    for index_w in range(weights.shape[0]):
        product = stacked[index_w]
        if index_w < rotated_count:
            product = rotate(product, offset, HD)
        results.append(product.astype(jnp.bfloat16))
    return tuple(results)


def attend(prompt_keys, prompt_vals, target_q, target_k, target_v):
    seq_count = target_q.shape[0]
    target_len = target_q.shape[1]
    prompt_len = prompt_keys.shape[0]
    heads_here = target_q.shape[2] // HD
    keys_all = jnp.concatenate([prompt_keys[None], target_k], axis=1)
    vals_all = jnp.concatenate([prompt_vals[None], target_v], axis=1)
    query_h = target_q.reshape(seq_count, target_len, heads_here, HD)
    key_h = keys_all.reshape(seq_count, prompt_len + target_len, heads_here, HD)
    val_h = vals_all.reshape(seq_count, prompt_len + target_len, heads_here, HD)
    scores = jnp.einsum(
        "bqhe,bkhe->bhqk", query_h, key_h, preferred_element_type=jnp.float32
    ) * HD ** (-0.5)
    key_index = jnp.arange(prompt_len + target_len, dtype=jnp.int32)
    query_pos = prompt_len + jnp.arange(target_len, dtype=jnp.int32)
    allowed = key_index[None, :] <= query_pos[:, None]
    scores = jnp.where(allowed[None, None], scores, -1e30)
    top_val = jnp.max(scores, axis=-1, keepdims=True)
    expo = jnp.exp(scores - top_val)
    probs = (expo / jnp.sum(expo, axis=-1, keepdims=True)).astype(jnp.bfloat16)
    context = jnp.einsum("bhqk,bkhe->bqhe", probs, val_h, preferred_element_type=jnp.float32)
    return context.astype(jnp.bfloat16).reshape(seq_count, target_len, heads_here * HD)


def block_stats(normed_rows, label_ids, columns, column_ids):
    logits = jnp.dot(normed_rows, columns, preferred_element_type=jnp.float32)
    top_val = jnp.max(logits, axis=1)
    sum_exp = jnp.sum(jnp.exp(logits - top_val[:, None]), axis=1)
    picked = jnp.sum(jnp.where(column_ids[None, :] == label_ids[:, None], logits, 0.0), axis=1)
    return (top_val, sum_exp, picked)


def combine_stats(earlier, later):
    top_val = jnp.maximum(earlier[0], later[0])
    sum_exp = earlier[1] * jnp.exp(earlier[0] - top_val) + later[1] * jnp.exp(later[0] - top_val)
    return (top_val, sum_exp, earlier[2] + later[2])


def shards(prompts, target_embed, labels, lengths, attn_gain, w_qkv, w_out, final_gain, w_vocab):
    n_prompt = lax.axis_size("prompt")
    n_model = lax.axis_size("mp")
    n_seq = lax.axis_size("dp")
    my_model = lax.axis_index("mp")
    my_seq = lax.axis_index("dp")
    prompts_here = prompts.shape[0]
    prompt_len = prompts.shape[1]
    seq_count = target_embed.shape[0]
    target_len = target_embed.shape[1]
    model_width = target_embed.shape[2]
    hops = range(1, n_model)
    out_pieces = [shift_by(peer_piece(w_out), "mp", k) for k in hops]
    out_mats = [w_out] + [spread_rows(piece, "prompt") for piece in out_pieces]
    total_rows = prompts_here * seq_count * target_len
    keep_rows = total_rows // n_model
    my_start = my_model * keep_rows
    label_rows = lax.dynamic_slice_in_dim(
        jnp.tile(labels.reshape(-1), prompts_here), my_start, keep_rows, 0
    )
    every_labels = small_gather(label_rows, "dp")

    normed_target = rms_scaled(target_embed, attn_gain).astype(jnp.bfloat16)
    target_q, target_k, target_v = project(normed_target, w_qkv, prompt_len, 2)
    normed_prompts = rms_scaled(prompts, attn_gain).astype(jnp.bfloat16)
    prompt_k, prompt_v = project(normed_prompts, w_qkv[1:], 0, 1)

    def one_prompt(pair):
        return attend(pair[0], pair[1], target_q, target_k, target_v)

    contexts = lax.map(one_prompt, (prompt_k, prompt_v))
    ctx_rows = contexts.reshape(-1, contexts.shape[-1])

    def rows_for(target):
        return lax.dynamic_slice_in_dim(ctx_rows, target * keep_rows, keep_rows, 0)

    ctx_parts = [rows_for(my_model)] + [
        shift_by(rows_for(lax.rem(my_model + k, n_model)), "mp", k) for k in hops
    ]
    embed_rows = jnp.tile(target_embed.reshape(-1, model_width), (prompts_here, 1))
    hidden = lax.dynamic_slice_in_dim(embed_rows, my_start, keep_rows, 0).astype(jnp.float32)
    for part, matrix in zip(ctx_parts, out_mats):
        head_part = jnp.dot(part, matrix, preferred_element_type=jnp.float32)
        hidden = hidden + head_part.astype(jnp.bfloat16).astype(jnp.float32)
    normed_out = rms_scaled(hidden, final_gain).astype(jnp.bfloat16)

    vocab_cols = w_vocab.shape[1]
    chunks = 2 if keep_rows % 32 == 0 else 1
    chunk_rows = keep_rows // chunks
    gathered = [
        lax.all_gather(normed_out[c * chunk_rows : (c + 1) * chunk_rows], "dp", axis=0, tiled=True)
        for c in range(chunks)
    ]
    vocab_own, normed_out = lax.optimization_barrier((peer_piece(w_vocab), normed_out))
    vocab_pieces = [shift_by(vocab_own, "mp", k) for k in hops]
    vocab_pieces, gathered[0] = lax.optimization_barrier((vocab_pieces, gathered[0]))
    vocab_mats = [w_vocab] + [spread_rows(piece, "prompt") for piece in vocab_pieces]
    chunk_stats = []
    for c in range(chunks):
        low = c * chunk_rows
        every_rows = gathered[c]
        chunk_labels = every_labels[:, low : low + chunk_rows].reshape(-1)
        merged = None
        for k, matrix in enumerate(vocab_mats):
            block_index = my_seq * n_model + ring_source("mp", k)
            column_ids = block_index * vocab_cols + jnp.arange(vocab_cols, dtype=jnp.int32)
            block = block_stats(every_rows, chunk_labels, matrix, column_ids)
            merged = block if merged is None else combine_stats(merged, block)
        chunk_stats.append(jnp.stack(merged).reshape(3, n_seq, chunk_rows))
    stats = jnp.concatenate(chunk_stats, axis=2)

    def stats_for(target):
        return lax.dynamic_index_in_dim(stats, target, 1, keepdims=False)

    merged = stats_for(my_seq)
    for k in range(1, n_seq):
        other = shift_by(stats_for(lax.rem(my_seq + k, n_seq)), "dp", k)
        merged = jnp.stack(combine_stats(merged, other))
    kept = merged[0] + jnp.log(merged[1]) - merged[2]
    losses = small_gather(kept, "mp").reshape(prompts_here, seq_count, target_len)
    valid = jnp.arange(target_len, dtype=jnp.int32)[None, :] < lengths[:, None]
    token_loss = jnp.where(valid[None], losses, 0.0)
    prompt_sums = jnp.sum(token_loss, axis=(1, 2))
    counted = jnp.sum(lengths).astype(jnp.float32)
    sums = jnp.sum(small_gather(jnp.concatenate([prompt_sums, counted[None]]), "dp"), axis=0)
    table = small_gather(sums, "prompt")
    prompt_loss = table[:, :prompts_here].reshape(-1) / table[0, prompts_here]
    return (token_loss, prompt_loss)


def solution(mesh):
    return jax.shard_map(
        shards,
        mesh=mesh,
        in_specs=(
            P("prompt", None, None),
            P("dp", None, None),
            P("dp", None),
            P("dp"),
            P(),
            P(None, None, "mp"),
            P("mp", None),
            P(),
            P(None, ("dp", "mp")),
        ),
        out_specs=(P("prompt", "dp", None), P()),
        check_vma=False,
    )
```
